256 devices in a mesh: pipe: 4 (over x), seq: 64 (over z, y, core).
Axes of the slice: x: 4, y: 4, z: 8, core: 2. Of those that a mesh axis runs over, the one named last changes fastest.
Arguments:
- previous: bfloat16 [4, 8192, 8192], P('pipe', 'seq'), may hold values from -6 to 6
- saved_head_inputs: bfloat16 [4, 8192, 8192], P('pipe', 'seq'), may hold values from -0.29882812 to 0.29882812
- input_b: bfloat16 [4, 8192, 1024], P('pipe', 'seq'), may hold values from -0.5 to 0.5
- input_c: bfloat16 [4, 8192, 1024], P('pipe', 'seq'), may hold values from -0.5 to 0.5
- steps: float32 [4, 8192, 128], P('pipe', 'seq'), may hold values from 0.1 to 13107.2, as said below
- decay_rate: float32 [4, 128], P('pipe'), may hold values from 3.0517578e-05 to 0.05
- skip_gain: float32 [4, 128], P('pipe'), may hold values from 0.5 to 1.5
- segment_ids: int32 [4, 8192], P('pipe', 'seq'), may hold values from 0 to 7, never falling along the last dimension, each value on 1 to 4096 neighbouring positions
- advantage_mask: int32 [8192], P('seq'), may hold values 0 or 1
Outputs:
- grad_x: bfloat16 [4, 8192, 8192], P('pipe', 'seq')
- grad_b: bfloat16 [4, 8192, 1024], P('pipe', 'seq')
- grad_c: bfloat16 [4, 8192, 1024], P('pipe', 'seq')
- bypass_gain_adjoint: float32 [4, 128], P('pipe')
The draws below stay inside these ranges and needn't reach their ends.
Inputs may be any that keep to these rules, and one draw needn't show every extreme that they name: `steps`: Positive; in a few positions of each section the step is 1.6 * 8192 for every head.
All inputs are finite; a program needn't handle non-finite values. No bound on the sum of `advantage_mask` on one device may be relied on, other than what follows from the above.
Results may differ from the reference program's by a relative error of at most 0.0095.
Values may be sent and summed in bfloat16 or wider, within the bound.
No kernel may reach another device: no remote copies, remote signals or barrier semaphores. Data moves between devices by JAX's collectives and lax.ppermute only.
A program may use at most 128 MiB of HBM per device.

```python
import math
import jax
import jax.numpy as jnp
import numpy as np
from jax import lax

HEADS = 128
HEAD_DIM = 64
STATE = 128
GROUPS = 8
BLOCK = 256
TOK_DEV = 128
MERGED_POSITIONS = 8192
N_PIPE = 4
N_SEQ = 64


def draw_steps(key, part):
    first, second, tertiary_multiplier = jax.random.split(key, 3)
    starting_position = jax.random.uniform(first, (N_PIPE, MERGED_POSITIONS, HEADS), jnp.float32, 0.5, 2.0)
    factor = jax.random.uniform(second, (N_PIPE, MERGED_POSITIONS // TOK_DEV, 1, 1), jnp.float32, 1.0, 2.5)
    starting_position = (starting_position.reshape(N_PIPE, MERGED_POSITIONS // TOK_DEV, TOK_DEV, HEADS) * factor).reshape(N_PIPE, MERGED_POSITIONS, HEADS)
    relay_interval = jax.random.randint(tertiary_multiplier, (N_PIPE, MERGED_POSITIONS, 1), 0, max(MERGED_POSITIONS // 4, 1)) == 0
    return jnp.where(relay_interval, jnp.float32(1.6 * MERGED_POSITIONS), starting_position)


def with_ends(entries, stream_key, low, top_value):
    longest = entries.shape.index(max(entries.shape))
    spots = []
    for shift in (0, 1):
        where = [jax.random.randint(jax.random.fold_in(stream_key, axis), (), 0, length) for axis, length in enumerate(entries.shape)]
        where[longest] = (where[longest] + shift) % entries.shape[longest]
        spots.append(tuple(where))
    return entries.at[spots[0]].set(low).at[spots[1]].set(top_value)


def levels(key, shape, cuts, low, high):
    level = 1.0
    for position, shards_of in cuts:
        heights = jax.random.uniform(jax.random.fold_in(jax.random.fold_in(key, 6), position), (shards_of,), jnp.float32, low / len(cuts), high / len(cuts))
        level = level * jnp.repeat(jnp.exp(heights), shape[position] // shards_of).reshape((-1,) + (1,) * (len(shape) - 1 - position))
    return level


def length_profile(count, total, bound, slope):
    portions = [(1 << 20) // math.isqrt(standing ** slope) + 1 for standing in range(2, count + 1)]
    spare, holding = total - bound - (count - 1), [1] * (count - 1)
    while spare > 0:
        free = [i for i in range(count - 1) if holding[i] < bound]
        pool, left = sum([portions[i] for i in free]), spare
        for i in free:
            more = min(bound - holding[i], max(1, left * portions[i] // pool), spare)
            holding[i] = holding[i] + more
            spare = spare - more
    return np.array([bound] + holding)


def ragged(own_key, number_of, total, most, lean):
    if number_of == 2:
        one = jax.random.randint(own_key, (), max(1, total - most), min(most, total - 1) + 1)
        return jnp.stack([one, total - one])
    lengths = jnp.asarray(length_profile(number_of, total, most, lean), jnp.int32)
    pairs = (number_of - 1) // 2
    donor, sink = lengths[1:1 + 2 * pairs:2], lengths[2:2 + 2 * pairs:2]
    margin = jnp.minimum(donor - 1, most - sink)
    shifted = jax.random.randint(jax.random.fold_in(own_key, 1), (pairs,), 0, 1 << 20) % (margin + 1)
    lengths = lengths.at[1:1 + 2 * pairs:2].set(donor - shifted).at[2:2 + 2 * pairs:2].set(sink + shifted)
    return lengths[jax.random.permutation(jax.random.fold_in(own_key, 2), number_of)]


def scatter_about(key, dims, deviation, most, cuts=(), dtype=jnp.bfloat16):
    loudness = levels(key, dims, cuts, -0.22, 0.18) if cuts else 1.0
    result = jax.random.normal(key, dims, jnp.float32) * deviation * loudness
    return jnp.minimum(jnp.maximum(result, -most), most).astype(dtype)


def setup_inputs(seed: int = 0) -> dict:
    arg_keys = jax.random.split(jax.random.key(seed), 10)
    return {
        "previous": scatter_about(arg_keys[0], (N_PIPE, MERGED_POSITIONS, HEADS * HEAD_DIM), 1.0, 6.0, ((0, 4), (1, 64))),
        "saved_head_inputs": scatter_about(arg_keys[1], (N_PIPE, MERGED_POSITIONS, HEADS * HEAD_DIM), 0.05, 0.29882812, ((0, 4), (1, 64))),
        "input_b": scatter_about(arg_keys[2], (N_PIPE, MERGED_POSITIONS, GROUPS * STATE), STATE ** -0.5, 0.5, ((0, 4), (1, 64))),
        "input_c": scatter_about(arg_keys[3], (N_PIPE, MERGED_POSITIONS, GROUPS * STATE), STATE ** -0.5, 0.5, ((0, 4), (1, 64))),
        "steps": draw_steps(jax.random.fold_in(arg_keys[9], 71), 0),
        "decay_rate": jnp.clip(jnp.exp(math.log(0.05) - 7.4014754 * jax.random.uniform(arg_keys[5], (N_PIPE, HEADS), jnp.float32) ** levels(arg_keys[5], (N_PIPE, HEADS), ((0, 4),), -0.2, 0.2)), 3.0517578125e-05, 0.05),
        "skip_gain": jnp.clip(1.0 + 0.1 * jax.random.normal(arg_keys[6], (N_PIPE, HEADS), jnp.float32), 0.5, 1.5),
        "segment_ids": jax.vmap(lambda own: jnp.searchsorted(jnp.cumsum(ragged(own, max(2, N_SEQ // 8), MERGED_POSITIONS, MERGED_POSITIONS // 2, 1)), jnp.arange(MERGED_POSITIONS), side="right"))(jax.random.split(arg_keys[7], N_PIPE)).reshape((N_PIPE, MERGED_POSITIONS)).astype(jnp.int32),
        "advantage_mask": with_ends((jax.random.randint(arg_keys[8], (MERGED_POSITIONS,), 0, 4) < 3).astype(jnp.int32), jax.random.fold_in(arg_keys[8], 1), 0, 1),
    }


def mix(form, left, right):
    return jnp.einsum(form, left.astype(jnp.float32), right.astype(jnp.float32))


def prepare(seg, prev, steps_here, rate):
    length = seg.shape[0]
    cum = jnp.cumsum(-steps_here * rate[None, :], axis=0)
    row = lax.broadcasted_iota(jnp.int32, (length, length), 0)
    col = lax.broadcasted_iota(jnp.int32, (length, length), 1)
    link = (seg[:, None] == seg[None, :]) & (row >= col)
    spread = cum[:, None, :] - cum[None, :, :]
    kernel = jnp.exp(jnp.where(link[:, :, None], spread, -1e30))
    enter = jnp.exp(cum) * (seg == prev)[:, None].astype(jnp.float32)
    leave = jnp.exp(cum[-1][None, :] - cum) * (seg == seg[-1])[:, None].astype(jnp.float32)
    through = jnp.exp(cum[-1]) * (seg[-1] == prev).astype(jnp.float32)
    return kernel, enter, leave, through


def block_states(grad4, inputs4, bmat, cmat, enter, leave):
    shape = grad4.shape
    xo = (leave.reshape(shape[0], shape[1], shape[2])[..., None] * inputs4).astype(jnp.bfloat16)
    gi = (enter.reshape(shape[0], shape[1], shape[2])[..., None] * grad4).astype(jnp.bfloat16)
    state = mix("tgkp,tgn->gkpn", xo, bmat)
    adjoint = mix("tgkp,tgn->gkpn", gi, cmat)
    return xo, gi, state, adjoint


def block_grads(grad4, inputs4, bmat, cmat, kernel, leave, xo, gi, entering_state, later, skip):
    length, groups, per_group, head_dim = grad4.shape
    kernel4 = kernel.reshape(length, length, groups, per_group)
    prod = mix("tgkp,ugkp->tugk", grad4, inputs4)
    w_one = (prod * kernel4).astype(jnp.bfloat16)
    cross = mix("tgn,ugn->tug", bmat, cmat)
    w_two = (jnp.swapaxes(kernel4, 0, 1) * cross[:, :, :, None]).astype(jnp.bfloat16)
    grad_c = mix("tugk,ugn->tgn", w_one, bmat) + mix("tgkp,gkpn->tgn", gi, entering_state)
    grad_b = mix("utgk,ugn->tgn", w_one, cmat) + mix("tgkp,gkpn->tgn", xo, later)
    leave4 = leave.reshape(length, groups, per_group)[..., None]
    grad_x = mix("tugk,ugkp->tgkp", w_two, grad4) + leave4 * mix("tgn,gkpn->tgkp", bmat, later)
    grad_x = grad_x + skip.reshape(groups, per_group)[None, :, :, None] * grad4.astype(jnp.float32)
    return grad_x, grad_b, grad_c


def section_backward(incoming, inputs_here, bmat_here, cmat_here, step_here, seg_here, rate, skip, groups, per_group):
    tokens = incoming.shape[0]
    heads = groups * per_group
    head_dim = incoming.shape[1] // heads
    blocks = tokens // BLOCK
    grads = incoming.reshape(blocks, BLOCK, groups, per_group, head_dim)
    inputs = inputs_here.reshape(blocks, BLOCK, groups, per_group, head_dim)
    bmats = bmat_here.reshape(blocks, BLOCK, groups, STATE)
    cmats = cmat_here.reshape(blocks, BLOCK, groups, STATE)
    segs = seg_here.reshape(blocks, BLOCK).astype(jnp.int32)
    prevs = jnp.concatenate([jnp.full((1,), -1, jnp.int32), segs[:-1, -1].astype(jnp.int32)])
    step_blocks = step_here.reshape(blocks, BLOCK, heads)

    def first_pass(item):
        seg, prev, steps_here, grad4, inputs4, bmat, cmat = item
        kernel, enter, leave, through = prepare(seg, prev, steps_here, rate)
        xo, gi, state, adjoint = block_states(grad4, inputs4, bmat, cmat, enter, leave)
        return through.reshape(groups, per_group), state, adjoint

    items = (segs, prevs, step_blocks, grads, inputs, bmats, cmats)
    through, states, adjoints = lax.map(first_pass, items)
    zeros = jnp.zeros((groups, per_group, head_dim, STATE), jnp.float32)

    def forward(carry, item):
        return carry * item[0][:, :, None, None] + item[1], carry

    def backward(carry, item):
        return item[1] + item[0][:, :, None, None] * carry, carry

    unused_one, entering_state = lax.scan(forward, zeros, (through, states))
    unused_two, later = lax.scan(backward, zeros, (through, adjoints), reverse=True)
    entering_state = entering_state.astype(jnp.bfloat16)
    later = later.astype(jnp.bfloat16)

    def second_pass(item):
        seg, prev, steps_here, grad4, inputs4, bmat, cmat, enter_state, later_state = item
        kernel, enter, leave, discarded_result = prepare(seg, prev, steps_here, rate)
        xo, gi, state, adjoint = block_states(grad4, inputs4, bmat, cmat, enter, leave)
        return block_grads(grad4, inputs4, bmat, cmat, kernel, leave, xo, gi, enter_state, later_state, skip)

    grad_x, grad_b, grad_c = lax.map(second_pass, items + (entering_state, later))
    return grad_x.reshape(tokens, heads * head_dim), grad_b.reshape(tokens, groups * STATE), grad_c.reshape(tokens, groups * STATE)


def reference(previous, saved_head_inputs, input_b, input_c, steps, decay_rate, skip_gain, segment_ids, advantage_mask):
    sections = previous.shape[0]
    tokens = previous.shape[1]
    heads = decay_rate.shape[1]
    head_dim = previous.shape[2] // heads
    groups = input_b.shape[2] // STATE
    per_group = heads // groups
    out_x, out_b, out_c, out_skip = [], [], [], []
    for section in range(sections):
        if section == sections - 1:
            incoming = previous[section] * advantage_mask.astype(jnp.bfloat16)[:, None]
        else:
            incoming = previous[section + 1]
        grad_x, grad_b, grad_c = section_backward(incoming, saved_head_inputs[section], input_b[section], input_c[section], steps[section], segment_ids[section], decay_rate[section], skip_gain[section], groups, per_group)
        out_x.append(grad_x.astype(jnp.bfloat16))
        out_b.append(grad_b.astype(jnp.bfloat16))
        out_c.append(grad_c.astype(jnp.bfloat16))
        out_skip.append(mix("thp,thp->h", incoming.reshape(tokens, heads, head_dim), saved_head_inputs[section].reshape(tokens, heads, head_dim)))
    return jnp.stack(out_x), jnp.stack(out_b), jnp.stack(out_c), jnp.stack(out_skip)
```

```python
import functools

import jax
import jax.numpy as jnp
from jax import lax
from jax.experimental import pallas as pl
from jax.experimental.pallas import tpu as pltpu
from jax.sharding import Mesh
from jax.sharding import PartitionSpec as P


CHIPS = ("seq_z", "seq_y")
F32 = jnp.float32
BF16 = jnp.bfloat16
LOG2E = 1.4426950408889634
TOK = 128
HALF = 4096
WIDE = 1024
PIECE = 80
CHUNKS = 2
PAIRS = 8


def dot_nn(left, right):
    return jnp.dot(left, right, preferred_element_type=F32)


def dot_nt(left, right):
    return lax.dot_general(left, right, (((1,), (1,)), ((), ())), preferred_element_type=F32)


def dot_tn(left, right):
    return lax.dot_general(left, right, (((0,), (0,)), ((), ())), preferred_element_type=F32)


def low_lanes(rows):
    return lax.broadcasted_iota(jnp.int32, (rows, 128), 1) < 64


def lanes_of(cols, pair, low):
    return jnp.where(low, cols[:, 2 * pair : 2 * pair + 1], cols[:, 2 * pair + 1 : 2 * pair + 2])


def scalars_of(ref, where, first, low):
    return jnp.where(low, ref[where, first], ref[where, first + 1])


def three_rows(value):
    value = jnp.broadcast_to(value, (16, 128))
    high = value.astype(BF16)
    rest = value - high.astype(F32)
    middle = rest.astype(BF16)
    low = (rest - middle.astype(F32)).astype(BF16)
    row = lax.broadcasted_iota(jnp.int32, (16, 128), 0)
    packed = jnp.where(row == 0, high.astype(F32), 0.0)
    packed = jnp.where(row == 1, middle.astype(F32), packed)
    return jnp.where(row == 2, low.astype(F32), packed).astype(BF16)


def from_three_rows(tile):
    return jnp.sum(tile.astype(F32), axis=0, keepdims=True)


def prep_kernel(meta, own, rec, seg, rate, cumc, cumr, ent, lea, th, m1, m2):
    first = meta[0] == 0
    prev = meta[1].astype(F32)
    row = lax.broadcasted_iota(jnp.int32, (TOK, TOK), 0)
    col = lax.broadcasted_iota(jnp.int32, (TOK, TOK), 1)
    tril = (row >= col).astype(F32)
    seg_own = seg[...]
    seg_rec = rec[TOK : TOK + 1, :]
    last_own, last_rec = seg_own[:, TOK - 1 :], seg_rec[:, TOK - 1 :]
    prev_own = jnp.where(first, jnp.full((1, 1), prev), last_rec)
    prev_rec = jnp.where(first, last_own, jnp.full((1, 1), prev))
    throughs = []
    for s, steps, segs, last, before in (
        (0, own[...], seg_own, last_own, prev_own),
        (1, rec[:TOK, :], seg_rec, last_rec, prev_rec),
    ):
        cum = (
            jnp.dot(
                tril,
                -(steps * rate[...]),
                precision=lax.Precision.HIGHEST,
                preferred_element_type=F32,
            )
            * LOG2E
        )
        cum = jnp.where(first, cum, pltpu.roll(cum, 64, 1))
        across = jnp.broadcast_to(segs, (TOK, TOK))
        down = across.T
        final = cum[TOK - 1 :, :]
        enter = jnp.where(down == before, jnp.exp2(cum), 0.0)
        leave = jnp.where(down == last, jnp.exp2(final - cum), 0.0)
        throughs.append(jnp.where(last == before, jnp.exp2(final), 0.0))
        heads_first = cum.T
        for g in range(4):
            cumr[s, g] = heads_first[16 * g : 16 * g + 16, :]
            cumc[s, g] = cum[:, 16 * g : 16 * g + 16]
            ent[s, g] = enter[:, 16 * g : 16 * g + 16]
            lea[s, g] = leave[:, 16 * g : 16 * g + 16]
        m1[s] = jnp.where((across == down) & (row >= col), 0.0, -1e30)
        m2[s] = jnp.where((across == down) & (row <= col), 0.0, -1e30)
    th[0:1, :] = jnp.where(first, throughs[0], throughs[1])
    th[1:2, :] = jnp.where(first, throughs[1], throughs[0])


def states_kernel(meta, x_own, x_rec, b_own, b_rec, lea, th, xo, first_state, pay):
    g = pl.program_id(0)
    first = meta[0] == 0
    low = low_lanes(TOK)
    for s, x in ((0, x_own), (1, x_rec)):
        cols = lea[s, 0]
        for p in range(PAIRS):
            at = slice(128 * p, 128 * p + 128)
            xo[s, :, at] = (lanes_of(cols, p, low) * x[:, at].astype(F32)).astype(BF16)
    own = dot_tn(b_own[...], xo[0])
    rec = dot_tn(b_rec[...], xo[1])
    for p in range(PAIRS):
        at = slice(128 * p, 128 * p + 128)
        early = jnp.where(first, own[:, at], rec[:, at])
        late = jnp.where(first, rec[:, at], own[:, at])
        t0 = scalars_of(th, 0, 16 * g + 2 * p, low)
        t1 = scalars_of(th, 1, 16 * g + 2 * p, low)
        first_state[:, at] = early.astype(BF16)
        total = (late + t1 * early).astype(BF16)
        extra = three_rows((t0 * t1)[0:1, :])
        for n in range(2):
            pay[2 * p + n, 0, 0:64, :] = total[64 * n : 64 * n + 64, :]
            pay[2 * p + n, 0, 64:80, :] = extra


def adjoints_kernel(
    meta, a_own, a_rec, m_own, m_rec, c_own, c_rec, x_own, x_rec, ent, th, gs, gi, late_state, pay, *, chunk
):
    g = pl.program_id(0)
    first = meta[0] == 0
    last_section = meta[2] == 1
    low = low_lanes(TOK)
    sums = [None] * PAIRS
    for s, a, m, x in ((0, a_own, m_own, x_own), (1, a_rec, m_rec, x_rec)):
        cols = ent[s, 0]
        for p in range(PAIRS):
            at = slice(128 * p, 128 * p + 128)
            grad = jnp.where(last_section, m[:, at].astype(F32), a[:, at].astype(F32))
            gs[s, :, at] = grad.astype(BF16)
            gi[s, :, at] = (lanes_of(cols, p, low) * grad).astype(BF16)
            part = jnp.sum(grad * x[:, at].astype(F32), axis=0, keepdims=True)
            sums[p] = part if s == 0 else sums[p] + part
    own = dot_tn(c_own[...], gi[0])
    rec = dot_tn(c_rec[...], gi[1])
    for p in range(PAIRS):
        at = slice(128 * p, 128 * p + 128)
        early = jnp.where(first, own[:, at], rec[:, at])
        late = jnp.where(first, rec[:, at], own[:, at])
        t0 = scalars_of(th, 0, 16 * (2 * chunk + g) + 2 * p, low)
        late_state[:, at] = late.astype(BF16)
        total = (early + t0 * late).astype(BF16)
        extra = three_rows(sums[p])
        for n in range(2):
            pay[2 * p + n, 0:64, :] = total[64 * n : 64 * n + 64, :]
            pay[2 * p + n, 64:80, :] = extra


def forward_scan_kernel(pay, out, decays):
    chips, per = pay.shape[0], pay.shape[1]
    for q in range(per):
        for c in range(CHUNKS):
            state = jnp.zeros((64, 128), F32)
            for j in range(chips):
                out[j, q, c] = state.astype(BF16)
                decay = from_three_rows(pay[j, q, c, 64:80, :])
                decays[c, q, j : j + 1, :] = decay
                state = pay[j, q, c, 0:64, :].astype(F32) + decay * state


def backward_scan_kernel(pay, decays, out, *, chunk):
    chips, per = pay.shape[0], pay.shape[1]
    for q in range(per):
        state = jnp.zeros((64, 128), F32)
        skip = jnp.zeros((1, 128), F32)
        for j in reversed(range(chips)):
            out[j, q, 0:64, :] = state.astype(BF16)
            state = pay[j, q, 0:64, :].astype(F32) + decays[chunk, q, j : j + 1, :] * state
            skip = skip + from_three_rows(pay[j, q, 64:80, :])
        extra = three_rows(skip)
        for j in range(chips):
            out[j, q, 64:80, :] = extra


def within_kernel(
    meta, gs, x_own, x_rec, b_own, b_rec, c_own, c_rec, cumc, cumr, m1, m2, skip, gx, gb, gc, *, chunk
):
    g = pl.program_id(0)
    head = 64 * meta[0] + 16 * (2 * chunk + g)
    low = low_lanes(TOK)
    mask_low = low.astype(F32).astype(BF16)
    mask_high = (1.0 - low.astype(F32)).astype(BF16)
    for s, x, b, c in ((0, x_own, b_own, c_own), (1, x_rec, b_rec, c_rec)):
        cross = dot_nt(b[...], c[...])
        lower, upper = m1[s], m2[s]
        cols, rows = cumc[s, 0], cumr[s, 0]
        total = jnp.zeros((TOK, TOK), F32)
        for p in range(PAIRS):
            at = slice(128 * p, 128 * p + 128)
            grad = gs[s, :, at]
            both = jnp.concatenate([grad * mask_low, grad * mask_high], axis=0)
            prod = dot_nt(both, x[:, at])
            weights = []
            for i in range(2):
                h = 2 * p + i
                spread = cols[:, h : h + 1] - rows[h : h + 1, :]
                total = total + prod[TOK * i : TOK * i + TOK, :] * jnp.exp2(spread + lower)
                weights.append((jnp.exp2(upper - spread) * cross).astype(BF16))
            mixed = dot_nn(jnp.concatenate(weights, axis=1), both)
            gains = jnp.where(low, skip[0, head + 2 * p], skip[0, head + 2 * p + 1])
            gx[s, :, at] = mixed + gains * grad.astype(F32)
        total = total.astype(BF16)
        gc[s] = dot_nn(total, b[...])
        gb[s] = dot_tn(total, c[...])


def final_kernel(
    meta, back_f, back_a, first_state, late_state, xo, gi, gx, gb, gc, b_own, b_rec, lea, th,
    x_out, b_out, c_out, ret, ent_s, lat_s, *, chunk
):
    g = pl.program_id(0)
    first = meta[0] == 0
    low = low_lanes(TOK)
    for p in range(PAIRS):
        at = slice(128 * p, 128 * p + 128)
        t0 = scalars_of(th, 0, 16 * (2 * chunk + g) + 2 * p, low)
        t1 = scalars_of(th, 1, 16 * (2 * chunk + g) + 2 * p, low)
        ent0 = jnp.concatenate([back_f[2 * p, 0], back_f[2 * p + 1, 0]], axis=0).astype(F32)
        ent1 = first_state[:, at].astype(F32) + t0 * ent0
        lat1 = jnp.concatenate([back_a[2 * p, 0:64, :], back_a[2 * p + 1, 0:64, :]], axis=0).astype(F32)
        lat0 = late_state[:, at].astype(F32) + t1 * lat1
        ent_s[0, :, at] = jnp.where(first, ent0, ent1).astype(BF16)
        ent_s[1, :, at] = jnp.where(first, ent1, ent0).astype(BF16)
        lat_s[0, :, at] = jnp.where(first, lat0, lat1).astype(BF16)
        lat_s[1, :, at] = jnp.where(first, lat1, lat0).astype(BF16)
    wide = pl.ds(pl.multiple_of(g * WIDE, WIDE), WIDE)
    for s, b in ((0, b_own), (1, b_rec)):
        grad_c = (gc[s] + dot_nt(gi[s], ent_s[s])).astype(BF16)
        grad_b = (gb[s] + dot_nt(xo[s], lat_s[s])).astype(BF16)
        spread = dot_nn(b[...], lat_s[s])
        cols = lea[s, 0]
        parts = []
        for p in range(PAIRS):
            at = slice(128 * p, 128 * p + 128)
            parts.append((gx[s, :, at] + lanes_of(cols, p, low) * spread[:, at]).astype(BF16))
        grad_x = jnp.concatenate(parts, axis=1)
        if s == 0:
            x_out[...] = grad_x
            b_out[...] = grad_b
            c_out[...] = grad_c
        else:
            ret[:, wide] = grad_x
            ret[:, pl.ds(pl.multiple_of(2 * WIDE + g * 128, 128), 128)] = grad_b
            ret[:, pl.ds(pl.multiple_of(2 * WIDE + 256 + g * 128, 128), 128)] = grad_c


def shape(dims, dtype):
    return jax.ShapeDtypeStruct(dims, dtype)


def smem():
    return pl.BlockSpec(memory_space=pltpu.SMEM)


def call(kernel, grid, in_specs, out_specs, out_shape, scratch=()):
    return pl.pallas_call(
        kernel,
        grid_spec=pltpu.PrefetchScalarGridSpec(
            num_scalar_prefetch=1,
            grid=grid,
            in_specs=in_specs,
            out_specs=out_specs,
            scratch_shapes=list(scratch),
        ),
        out_shape=out_shape,
        compiler_params=pltpu.CompilerParams(vmem_limit_bytes=40 * 1024 * 1024),
    )


def on_device(previous, saved, input_b, input_c, steps, decay_rate, skip_gain, segment_ids, advantage_mask):
    section = lax.axis_index("pipe")
    sections = lax.axis_size("pipe")
    k = lax.axis_index("seq_k")
    chip = lax.axis_index(CHIPS)
    chips = lax.axis_size(CHIPS)
    per = 32 // chips
    grad, x, b, c = previous[0], saved[0], input_b[0], input_c[0]

    def half(array, which):
        width = array.shape[1] // 2
        return lax.dynamic_slice_in_dim(array, which * width, width, 1)

    straight = [((p + 1) * 2 + i, p * 2 + i) for p in range(sections - 1) for i in range(2)]
    crossed = [((p + 1) * 2 + i, p * 2 + 1 - i) for p in range(sections - 1) for i in range(2)]
    mine, others = half(grad, k), half(grad, 1 - k)
    step = HALF // CHUNKS
    arrived = []
    for n in range(CHUNKS):
        arrived.append(
            (
                lax.ppermute(mine[:, n * step : (n + 1) * step], ("pipe", "seq_k"), straight),
                lax.ppermute(others[:, n * step : (n + 1) * step], ("pipe", "seq_k"), crossed),
            )
        )
    mask = advantage_mask.astype(BF16)[:, None]
    partner = [(0, 1), (1, 0)]
    numbers = segment_ids.astype(F32)
    packed = jnp.concatenate([steps[0], jnp.broadcast_to(numbers, (8, TOK))], axis=0)
    packed = lax.ppermute(packed, "seq_k", partner)
    bundle = jnp.concatenate(
        [half(x, 1 - k), half(b, 1 - k), half(c, 1 - k), others * mask], axis=1
    )
    bundle = lax.ppermute(bundle, "seq_k", partner)
    masked = mine * mask
    seq = CHIPS + ("seq_k",)
    ends = numbers
    by_one = lax.ppermute(ends, seq, [(i, i + 1) for i in range(2 * chips - 1)])
    by_two = lax.ppermute(ends, seq, [(i, i + 2) for i in range(2 * chips - 2)])
    before = jnp.where(k == 0, by_one[0, TOK - 1], by_two[0, TOK - 1])
    before = jnp.where(chip == 0, -1, before.astype(jnp.int32))
    meta = jnp.stack([k, before, (section == sections - 1).astype(jnp.int32)])

    full = lambda *dims: pl.BlockSpec(dims, lambda *_: (0,) * len(dims))
    cols = shape((2, 4, TOK, 16), F32)
    square = shape((2, TOK, TOK), F32)
    cumc, cumr, ent, lea, th, m1, m2 = call(
        prep_kernel,
        (1,),
        [full(TOK, 128), full(TOK + 8, 128), full(1, TOK), full(1, 128)],
        [
            full(2, 4, TOK, 16), full(2, 4, 16, TOK), full(2, 4, TOK, 16), full(2, 4, TOK, 16),
            full(2, 128), full(2, TOK, TOK), full(2, TOK, TOK),
        ],
        [cols, shape((2, 4, 16, TOK), F32), cols, cols, shape((2, 128), F32), square, square],
    )(meta, steps[0], packed, numbers, decay_rate)

    def wide_own(n):
        return pl.BlockSpec((TOK, WIDE), lambda g, m: (0, 4 * m[0] + 2 * n + g))

    def wide_at(n):
        return pl.BlockSpec((TOK, WIDE), lambda g, m: (0, n + g))

    def thin_own(n):
        return pl.BlockSpec((TOK, 128), lambda g, m: (0, 4 * m[0] + 2 * n + g))

    def thin_at(n):
        return pl.BlockSpec((TOK, 128), lambda g, m: (0, n + g))

    def two_at(n):
        return pl.BlockSpec((2, TOK, WIDE), lambda g, m: (0, 0, n + g))

    def cols_at(n):
        return pl.BlockSpec((2, 1, TOK, 16), lambda g, m: (0, n + g, 0, 0))

    xo, first_state, pay = call(
        states_kernel,
        (4,),
        [wide_own(0), wide_at(0), thin_own(0), thin_at(32), cols_at(0), smem()],
        [
            two_at(0),
            wide_at(0),
            pl.BlockSpec((16, 1, PIECE, 128), lambda g, m: (g % 2, g // 2, 0, 0)),
        ],
        [
            shape((2, TOK, HALF), BF16),
            shape((TOK, HALF), BF16),
            shape((32, CHUNKS, PIECE, 128), BF16),
        ],
    )(meta, x, bundle, b, bundle, lea, th)

    def to_all(array):
        return lax.all_to_all(array, CHIPS, split_axis=0, concat_axis=0, tiled=True)

    pay = to_all(pay.reshape(chips, per, CHUNKS, PIECE, 128))
    back_f, decays = pl.pallas_call(
        forward_scan_kernel,
        out_shape=[
            shape((chips, per, CHUNKS, 64, 128), BF16),
            shape((CHUNKS, per, chips, 128), F32),
        ],
    )(pay)
    back_f = to_all(back_f).reshape(32, CHUNKS, 64, 128)

    results = []
    for n in range(CHUNKS):
        a_own, a_rec = arrived[n]
        gs, gi, late_state, pay = call(
            functools.partial(adjoints_kernel, chunk=n),
            (2,),
            [
                wide_at(0), wide_at(0), wide_at(2 * n), wide_at(5 + 2 * n),
                thin_own(n), thin_at(36 + 2 * n), wide_own(n), wide_at(2 * n),
                cols_at(2 * n), smem(),
            ],
            [
                two_at(0), two_at(0), wide_at(0),
                pl.BlockSpec((16, PIECE, 128), lambda g, m: (g, 0, 0)),
            ],
            [
                shape((2, TOK, step), BF16), shape((2, TOK, step), BF16),
                shape((TOK, step), BF16), shape((32, PIECE, 128), BF16),
            ],
        )(meta, a_own, a_rec, masked, bundle, c, bundle, x, bundle, ent, th)
        pay = to_all(pay.reshape(chips, per, PIECE, 128))
        back_a = pl.pallas_call(
            functools.partial(backward_scan_kernel, chunk=n),
            out_shape=shape((chips, per, PIECE, 128), BF16),
        )(pay, decays)
        back_a = to_all(back_a).reshape(32, PIECE, 128)
        two_thin = pl.BlockSpec((2, TOK, 128), lambda g, m: (0, 0, g))
        rows_at = pl.BlockSpec((2, 1, 16, TOK), lambda g, m: (0, 2 * n + g, 0, 0))
        gx, gb, gc = call(
            functools.partial(within_kernel, chunk=n),
            (2,),
            [
                two_at(0), wide_own(n), wide_at(2 * n), thin_own(n), thin_at(32 + 2 * n),
                thin_own(n), thin_at(36 + 2 * n), cols_at(2 * n), rows_at,
                full(2, TOK, TOK), full(2, TOK, TOK), smem(),
            ],
            [two_at(0), two_thin, two_thin],
            [shape((2, TOK, step), F32), shape((2, TOK, 256), F32), shape((2, TOK, 256), F32)],
        )(meta, gs, x, bundle, b, bundle, c, bundle, cumc, cumr, m1, m2, skip_gain)
        x_out, b_out, c_out, ret = call(
            functools.partial(final_kernel, chunk=n),
            (2,),
            [
                pl.BlockSpec((16, 1, 64, 128), lambda g, m, n=n: (g, n, 0, 0)),
                pl.BlockSpec((16, PIECE, 128), lambda g, m: (g, 0, 0)),
                wide_at(2 * n), wide_at(0), two_at(2 * n), two_at(0), two_at(0), two_thin, two_thin,
                thin_own(n), thin_at(32 + 2 * n), cols_at(2 * n), smem(),
            ],
            [wide_at(0), thin_at(0), thin_at(0), full(TOK, step + 512)],
            [
                shape((TOK, step), BF16), shape((TOK, 256), BF16), shape((TOK, 256), BF16),
                shape((TOK, step + 512), BF16),
            ],
            [pltpu.VMEM((2, TOK, WIDE), BF16), pltpu.VMEM((2, TOK, WIDE), BF16)],
        )(meta, back_f, back_a, first_state, late_state, xo, gi, gx, gb, gc, b, bundle, lea, th)
        ret = lax.ppermute(ret, "seq_k", partner)
        sums = jnp.sum(back_a[0::2, 64:67, :].astype(F32), axis=1).reshape(32, 64).sum(axis=1)
        results.append((x_out, b_out, c_out, ret, sums))

    def ordered(own, rec):
        return jnp.where(k == 0, jnp.concatenate([own, rec], -1), jnp.concatenate([rec, own], -1))

    grad_x = ordered(
        jnp.concatenate([r[0] for r in results], 1), jnp.concatenate([r[3][:, :step] for r in results], 1)
    )
    grad_b = ordered(
        jnp.concatenate([r[1] for r in results], 1),
        jnp.concatenate([r[3][:, step : step + 256] for r in results], 1),
    )
    grad_c = ordered(
        jnp.concatenate([r[2] for r in results], 1),
        jnp.concatenate([r[3][:, step + 256 :] for r in results], 1),
    )
    sums = jnp.concatenate([r[4] for r in results])[None, :]
    adjoint = ordered(sums, lax.ppermute(sums, "seq_k", partner))
    return grad_x[None], grad_b[None], grad_c[None], adjoint


def solution(mesh):
    names = ("pipe", "seq_z", "seq_y", "seq_k")
    sizes = (mesh.shape["pipe"], mesh.shape["seq"] // 8, 4, 2)
    finer = Mesh(mesh.devices.reshape(sizes), names)
    seq = names[1:]
    by_token = P("pipe", seq, None)
    return jax.shard_map(
        on_device,
        mesh=finer,
        in_specs=(
            by_token, by_token, by_token, by_token, by_token,
            P("pipe", None), P("pipe", None), P("pipe", seq), P(seq),
        ),
        out_specs=(by_token, by_token, by_token, P("pipe", None)),
        check_vma=False,
    )
```
